32 devices in a mesh: dp: 2 (over x), tp: 4 (over z), sp: 4 (over y, core).
Axes of the slice: x: 2, y: 2, z: 4, core: 2. Of those that a mesh axis runs over, the one named last changes fastest.
Arguments:
- x: bfloat16 [4096, 4096], P(('dp', 'sp')), parts along dimension 0
- pos: int32 [4096], P(('dp', 'sp')), parts along dimension 0
- k_hist: bfloat16 [2, 16384, 8, 128], P(None, ('dp', 'sp'), 'tp'), parts along dimension 1
- v_hist: bfloat16 [2, 16384, 8, 128], P(None, ('dp', 'sp'), 'tp'), parts along dimension 1
- wq: bfloat16 [2, 4096, 4096], P(None, None, 'tp')
- wk: bfloat16 [2, 4096, 1024], P(None, None, 'tp')
- wv: bfloat16 [2, 4096, 1024], P(None, None, 'tp')
- wo: bfloat16 [2, 4096, 4096], P(None, 'tp')
- wg: bfloat16 [2, 4096, 14336], P(None, None, 'tp')
- wu: bfloat16 [2, 4096, 14336], P(None, None, 'tp')
- wd: bfloat16 [2, 14336, 4096], P(None, 'tp')
- g1: bfloat16 [2, 4096], replicated
- g2: bfloat16 [2, 4096], replicated
Outputs:
- output 1: bfloat16 [4096, 4096], P(('dp', 'sp')), parts along dimension 0
- output 2: bfloat16 [2, 4096, 8, 128], P(None, ('dp', 'sp'), 'tp'), parts along dimension 1
- output 3: bfloat16 [2, 4096, 8, 128], P(None, ('dp', 'sp'), 'tp'), parts along dimension 1
There are 2 independent parts. The reference program is written for one: setup_inputs(seed, part) draws one part's arguments, and reference() takes and returns one part's arrays. A program takes and returns all parts, laid end to end along the dimension named above; an argument that names none is the same for every part.
All inputs are finite; a program needn't handle non-finite values.
Results may differ from the reference program's by a relative error of at most 0.02.
Values are sent between devices in bfloat16 or wider.
A program may use at most 1 GiB of HBM per device.

```python
import jax
import jax.numpy as jnp
from jax import lax

D = 4096
HEADS = 32
KV_HEADS = 8
HEAD = 128
FF = 14336
S = 2048
HIST = 8192
LAYERS = 2
QBLK = 32
EPS = 1e-5
ROPE_THETA = 500000.0


def setup_inputs(seed: int = 0, part: int = 0) -> dict:
    key = jax.random.PRNGKey(seed)
    ks = jax.random.split(key, 9)
    kp = jax.random.split(jax.random.fold_in(key, part), 4)
    f32 = jnp.float32

    def w(k, shape, fan_in, gain=1.0):
        return (jax.random.normal(k, shape, f32) * (gain * fan_in ** -0.5)).astype(jnp.bfloat16)

    off = jax.random.randint(kp[1], (), 0, 1024)
    kvshape = (LAYERS, HIST, KV_HEADS, HEAD)
    return {
        'x': jax.random.normal(kp[0], (S, D), f32).astype(jnp.bfloat16),
        'pos': (HIST + off + jnp.arange(S)).astype(jnp.int32),
        'k_hist': jax.random.normal(kp[2], kvshape, f32).astype(jnp.bfloat16),
        'v_hist': jax.random.normal(kp[3], kvshape, f32).astype(jnp.bfloat16),
        'wq': w(ks[0], (LAYERS, D, HEADS * HEAD), D, 3.0),
        'wk': w(ks[1], (LAYERS, D, KV_HEADS * HEAD), D),
        'wv': w(ks[2], (LAYERS, D, KV_HEADS * HEAD), D),
        'wo': w(ks[3], (LAYERS, HEADS * HEAD, D), HEADS * HEAD),
        'wg': w(ks[4], (LAYERS, D, FF), D),
        'wu': w(ks[5], (LAYERS, D, FF), D),
        'wd': w(ks[6], (LAYERS, FF, D), FF),
        'g1': (1.0 + 0.2 * jax.random.normal(ks[7], (LAYERS, D), f32)).astype(jnp.bfloat16),
        'g2': (1.0 + 0.2 * jax.random.normal(ks[8], (LAYERS, D), f32)).astype(jnp.bfloat16),
    }


def rmsnorm(x, g):
    xf = x.astype(jnp.float32)
    r = lax.rsqrt(jnp.mean(xf * xf, axis=-1, keepdims=True) + EPS)
    return (xf * r * g.astype(jnp.float32)).astype(jnp.bfloat16)


def rope(t, pos):
    half = t.shape[-1] // 2
    inv = ROPE_THETA ** (-(jnp.arange(half, dtype=jnp.float32) * (2.0 / t.shape[-1])))
    ang = pos.astype(jnp.float32)[..., None] * inv
    c = jnp.cos(ang)[..., None, :]
    s = jnp.sin(ang)[..., None, :]
    tf = t.astype(jnp.float32)
    t1 = tf[..., :half]
    t2 = tf[..., half:]
    return jnp.concatenate([t1 * c - t2 * s, t2 * c + t1 * s], axis=-1).astype(jnp.bfloat16)


def attention(q, k, v):
    g = HEADS // KV_HEADS
    kf = k.astype(jnp.float32)
    vf = v.astype(jnp.float32)
    qb = q.reshape(S // QBLK, QBLK, KV_HEADS, g, HEAD)
    kidx = jnp.arange(HIST + S)

    def blk(args):
        i, qq = args
        s = jnp.einsum('qkgd,tkd->qkgt', qq.astype(jnp.float32), kf) * HEAD ** -0.5
        qidx = HIST + i * QBLK + jnp.arange(QBLK)
        mask = (kidx[None, :] <= qidx[:, None])[:, None, None, :]
        s = jnp.where(mask, s, -jnp.inf)
        p = jax.nn.softmax(s, axis=-1).astype(jnp.bfloat16)
        o = jnp.einsum('qkgt,tkd->qkgd', p.astype(jnp.float32), vf)
        return o.astype(jnp.bfloat16)

    o = lax.map(blk, (jnp.arange(S // QBLK), qb))
    return o.reshape(S, HEADS * HEAD)


def reference(x, pos, k_hist, v_hist, wq, wk, wv, wo, wg, wu, wd, g1, g2):
    def layer(x, w):
        kh, vh, wq_, wk_, wv_, wo_, wg_, wu_, wd_, g1_, g2_ = w
        h = rmsnorm(x, g1_)
        q = jnp.dot(h, wq_, preferred_element_type=jnp.float32).astype(jnp.bfloat16).reshape(S, HEADS, HEAD)
        k = jnp.dot(h, wk_, preferred_element_type=jnp.float32).astype(jnp.bfloat16).reshape(S, KV_HEADS, HEAD)
        v = jnp.dot(h, wv_, preferred_element_type=jnp.float32).astype(jnp.bfloat16).reshape(S, KV_HEADS, HEAD)
        q = rope(q, pos)
        k = rope(k, pos)
        a = attention(q, jnp.concatenate([kh, k], axis=0), jnp.concatenate([vh, v], axis=0))
        x = x + jnp.dot(a, wo_, preferred_element_type=jnp.float32).astype(jnp.bfloat16)
        h2 = rmsnorm(x, g2_)
        ga = jnp.dot(h2, wg_, preferred_element_type=jnp.float32).astype(jnp.bfloat16)
        up = jnp.dot(h2, wu_, preferred_element_type=jnp.float32).astype(jnp.bfloat16)
        u = (jax.nn.silu(ga.astype(jnp.float32)) * up.astype(jnp.float32)).astype(jnp.bfloat16)
        x = x + jnp.dot(u, wd_, preferred_element_type=jnp.float32).astype(jnp.bfloat16)
        return x, (k, v)

    x, (kn, vn) = lax.scan(layer, x, (k_hist, v_hist, wq, wk, wv, wo, wg, wu, wd, g1, g2))
    return x, kn, vn
```

```python
import functools

import jax
import jax.numpy as jnp
from jax import lax
from jax.experimental import pallas as pl
from jax.experimental.pallas import tpu as pltpu
from jax.sharding import PartitionSpec as P


EPS = 1e-5
ROPE_THETA = 500000.0
MESH = pl.DeviceIdType.MESH
LOG2E = 1.4426950408889634


def rope_tables(pos, dh):
    half = dh // 2
    inv = ROPE_THETA ** (-(jnp.arange(half, dtype=jnp.float32) * (2.0 / dh)))
    ang = pos.astype(jnp.float32)[:, None] * inv
    c, s = jnp.cos(ang), jnp.sin(ang)
    return jnp.concatenate([c, c], -1), jnp.concatenate([-s, s], -1)


def norm_into(x_ref, g_ref, h_ref):
    rb = 64
    for lo in range(0, x_ref.shape[0], rb):
        xf = x_ref[lo:lo + rb, :].astype(jnp.float32)
        r = lax.rsqrt(jnp.mean(xf * xf, axis=-1, keepdims=True) + EPS)
        h_ref[lo:lo + rb, :] = (xf * r * g_ref[...].astype(jnp.float32)).astype(jnp.bfloat16)


def qkv_kernel(nq, dh, x_ref, g_ref, c_ref, s_ref, wq_ref, wk_ref, wv_ref, q_ref, k_ref, v_ref, h_ref):
    i = pl.program_id(0)

    @pl.when(i == 0)
    def _():
        norm_into(x_ref, g_ref, h_ref)

    def rotated(w_ref, out):
        t = jnp.dot(h_ref[...], w_ref[...], preferred_element_type=jnp.float32)
        t = t.astype(jnp.bfloat16).astype(jnp.float32)
        for j in range(t.shape[1] // dh):
            th = t[:, j * dh:(j + 1) * dh]
            r = th * c_ref[...] + pltpu.roll(th, dh // 2, 1) * s_ref[...]
            out[:, j * dh:(j + 1) * dh] = r.astype(jnp.bfloat16)

    @pl.when(i < nq)
    def _():
        rotated(wq_ref, q_ref)

    @pl.when(i == nq)
    def _():
        rotated(wk_ref, k_ref)

    @pl.when(i == nq + 1)
    def _():
        v_ref[...] = jnp.dot(h_ref[...], wv_ref[...], preferred_element_type=jnp.float32).astype(jnp.bfloat16)


def qkv(x, g, c, s, wq, wk, wv, layer, dh):
    n, d = x.shape
    hq, hk = wq.shape[2], wk.shape[2]
    nc = 256
    nq = hq // nc
    vm = pl.BlockSpec(memory_space=pltpu.VMEM)
    bf = jnp.bfloat16
    return pl.pallas_call(
        functools.partial(qkv_kernel, nq, dh), grid=(nq + 2,),
        in_specs=[vm, vm, vm, vm,
                  pl.BlockSpec((None, d, nc), lambda i: (layer, 0, jnp.minimum(i, nq - 1))),
                  pl.BlockSpec((None, d, hk), lambda i: (layer, 0, 0)),
                  pl.BlockSpec((None, d, hk), lambda i: (layer, 0, 0))],
        out_specs=[pl.BlockSpec((n, nc), lambda i: (0, jnp.minimum(i, nq - 1))), vm, vm],
        out_shape=[jax.ShapeDtypeStruct((n, hq), bf), jax.ShapeDtypeStruct((n, hk), bf),
                   jax.ShapeDtypeStruct((n, hk), bf)],
        scratch_shapes=[pltpu.VMEM((n, d), bf)],
        cost_estimate=pl.CostEstimate(flops=2 * n * d * (hq + 2 * hk), bytes_accessed=2 * d * hq, transcendentals=0),
        compiler_params=pltpu.CompilerParams(vmem_limit_bytes=48 * 1024 * 1024),
        name="qkv",
    )(x, g, c, s, wq, wk, wv)


def gate_kernel(x_ref, g_ref, wg_ref, wu_ref, u_ref, h_ref):
    @pl.when(pl.program_id(0) == 0)
    def _():
        norm_into(x_ref, g_ref, h_ref)

    a = jnp.dot(h_ref[...], wg_ref[...], preferred_element_type=jnp.float32)
    b = jnp.dot(h_ref[...], wu_ref[...], preferred_element_type=jnp.float32)
    a = a.astype(jnp.bfloat16).astype(jnp.float32)
    b = b.astype(jnp.bfloat16).astype(jnp.float32)
    u_ref[...] = (jax.nn.silu(a) * b).astype(jnp.bfloat16)


def gate_up(x, g, wg, wu, layer):
    n, d = x.shape
    f = wg.shape[2]
    nc = 256
    vm = pl.BlockSpec(memory_space=pltpu.VMEM)
    wspec = pl.BlockSpec((None, d, nc), lambda i: (layer, 0, i))
    return pl.pallas_call(
        gate_kernel, grid=(f // nc,), in_specs=[vm, vm, wspec, wspec],
        out_specs=pl.BlockSpec((n, nc), lambda i: (0, i)),
        out_shape=jax.ShapeDtypeStruct((n, f), jnp.bfloat16),
        scratch_shapes=[pltpu.VMEM((n, d), jnp.bfloat16)],
        cost_estimate=pl.CostEstimate(flops=4 * n * d * f, bytes_accessed=4 * d * f, transcendentals=0),
        compiler_params=pltpu.CompilerParams(vmem_limit_bytes=48 * 1024 * 1024),
        name="gate_up",
    )(x, g, wg, wu)


def attn_kernel(nfull, ncond, diag, first, last, ntp, heads, scale, rb, tk, *refs):
    it = iter(refs)
    bias = next(it)
    q_ref = next(it)
    full = [(next(it), next(it)) for _ in range(nfull)]
    own = (next(it), next(it)) if diag else None
    cond = [(next(it), next(it)) for _ in range(ncond)]
    if not first:
        m_in, l_in, o_in = next(it), next(it), next(it)
    out = next(it)
    if not last:
        m_s, l_s, o_s = out, next(it), next(it)
    nq = q_ref.shape[0]
    rows = range(0, nq, rb)

    def logits(t):
        lo, k_ref, _, off, size, _ = t
        s = lax.dot_general(q_ref[lo:lo + rb, :], k_ref[off:off + size, :], (((1,), (1,)), ((), ())),
                            preferred_element_type=jnp.float32)
        return s * (scale * LOG2E)

    def absorb(t, s, st):
        lo, _, v_ref, off, size, mask = t
        if mask == "causal":
            r = lax.broadcasted_iota(jnp.int32, s.shape, 0) + lo
            c = lax.broadcasted_iota(jnp.int32, s.shape, 1) + off
            s = jnp.where(c <= r, s, -jnp.inf)
        elif mask == "bias":
            s = s + bias[:1, off:off + size]
        mx = jnp.max(s, axis=-1, keepdims=True)
        if st is not None:
            mx = jnp.maximum(mx, st[0])
        p = jnp.exp2(s - mx)
        ps = jnp.sum(p, axis=-1, keepdims=True)
        o = jnp.dot(p.astype(jnp.bfloat16), v_ref[off:off + size, :], preferred_element_type=jnp.float32)
        if st is not None:
            al = jnp.exp2(st[0] - mx)
            ps = ps + al * st[1]
            o = o + al * st[2]
        return mx, ps, o

    def one_head(put):
        st = {lo: None for lo in rows}
        if not first:
            st = {lo: (m_in[lo:lo + rb, :1], l_in[lo:lo + rb, :1], o_in[lo:lo + rb, :]) for lo in rows}
        tiles = [(lo, k, v, off, tk, None) for k, v in full for off in range(0, k.shape[0], tk) for lo in rows]
        if diag:
            tiles += [(lo, own[0], own[1], 0, lo + rb, "causal") for lo in rows]
        tiles += [(lo, k, v, 0, k.shape[0], "bias") for k, v in cond for lo in rows]
        s_next = logits(tiles[0])
        for i, t in enumerate(tiles):
            s = s_next
            if i + 1 < len(tiles):
                s_next = logits(tiles[i + 1])
            st[t[0]] = absorb(t, s, st[t[0]])
        for lo in rows:
            m, l, o = st[lo]
            if last:
                put(lo, (o / l).astype(jnp.bfloat16))
            else:
                m_s[lo:lo + rb, :] = jnp.broadcast_to(m, (rb, 128))
                l_s[lo:lo + rb, :] = jnp.broadcast_to(l, (rb, 128))
                o_s[lo:lo + rb, :] = o

    if ntp == 1:
        def put(lo, v):
            out[lo:lo + rb, :] = v

        one_head(put)
        return

    buf, send_r, send_l, recv_r, recv_l = [next(it) for _ in range(5)]
    z = lax.axis_index("tp")
    step = pl.program_id(0)
    end = ntp - 1
    dh = q_ref.shape[1]

    @pl.when(step == 0)
    def _():
        bar = pltpu.get_barrier_semaphore()

        @pl.when(z > 0)
        def _():
            pl.semaphore_signal(bar, inc=1, device_id={"tp": z - 1}, device_id_type=MESH)

        @pl.when(z < end)
        def _():
            pl.semaphore_signal(bar, inc=1, device_id={"tp": z + 1}, device_id_type=MESH)

        @pl.when((z > 0) & (z < end))
        def _():
            pl.semaphore_wait(bar, 2)

        @pl.when((z == 0) | (z == end))
        def _():
            pl.semaphore_wait(bar, 1)

    def rightwards(src, h):
        return pltpu.make_async_remote_copy(
            src_ref=buf.at[src, h], dst_ref=buf.at[src, h], send_sem=send_r.at[src, h], recv_sem=recv_r.at[src, h],
            device_id={"tp": z + 1}, device_id_type=MESH)

    def leftwards(src, h):
        return pltpu.make_async_remote_copy(
            src_ref=buf.at[src, h], dst_ref=buf.at[src, h], send_sem=send_l.at[src, h], recv_sem=recv_l.at[src, h],
            device_id={"tp": z - 1}, device_id_type=MESH)

    def emit(src, h):
        col = pl.multiple_of((h * ntp + src) * dh, dh)
        out[:, pl.ds(col, dh)] = buf[src, h]

    @pl.when(step < heads)
    def _():
        def put(lo, v):
            buf[z, step, lo:lo + rb, :] = v

        one_head(put)

        @pl.when(z < end)
        def _():
            rightwards(z, step).start()

        @pl.when(z > 0)
        def _():
            leftwards(z, step).start()

        emit(z, step)

    for k in range(1, ntp):
        c = step - k
        live = (c >= 0) & (c < heads)

        @pl.when(live & (z - k >= 0))
        def _():
            rightwards(z - k, c).wait_recv()

            @pl.when(z < end)
            def _():
                rightwards(z - k, c).start()

            emit(z - k, c)

        @pl.when(live & (z + k <= end))
        def _():
            leftwards(z + k, c).wait_recv()

            @pl.when(z > 0)
            def _():
                leftwards(z + k, c).start()

            emit(z + k, c)

    @pl.when(step == pl.num_programs(0) - 1)
    def _():
        def body(h, _):
            for src in range(ntp):
                @pl.when((z >= src) & (z < end))
                def _():
                    rightwards(src, h).wait_send()

                @pl.when((z <= src) & (z > 0))
                def _():
                    leftwards(src, h).wait_send()
            return 0

        lax.fori_loop(0, heads, body, 0)


def attention(bias, q, full, diag, cond, state, last, g, ntp=1, cid=None):
    n, hd = q.shape
    dh = 128
    heads = hd // dh
    first = state is None
    steps = heads if ntp == 1 else heads + ntp - 1
    at = lambda h: jnp.minimum(h, heads - 1)
    args = [bias, q]
    specs = [pl.BlockSpec(memory_space=pltpu.VMEM), pl.BlockSpec((n, dh), lambda h: (0, at(h)))]
    kvspec = lambda t: pl.BlockSpec((t, dh), lambda h: (0, at(h) // g))
    keys = 0
    for k, v in full + ([diag] if diag is not None else []) + cond:
        args += [k, v]
        specs += [kvspec(k.shape[0])] * 2
        keys += k.shape[0]
    hspec = pl.BlockSpec((n, dh), lambda h: (0, at(h)))
    f32 = jax.ShapeDtypeStruct((n, hd), jnp.float32)
    if not first:
        args += list(state)
        specs += [hspec] * 3
    scratch = []
    if ntp > 1:
        out_shape = jax.ShapeDtypeStruct((n, hd * ntp), jnp.bfloat16)
        out_specs = pl.BlockSpec(memory_space=pltpu.VMEM)
        scratch = [pltpu.VMEM((ntp, heads, n, dh), jnp.bfloat16)] + [pltpu.SemaphoreType.DMA((ntp, heads))] * 4
    elif last:
        out_shape, out_specs = jax.ShapeDtypeStruct((n, hd), jnp.bfloat16), hspec
    else:
        out_shape, out_specs = (f32,) * 3, (hspec,) * 3
    kern = functools.partial(attn_kernel, len(full), len(cond), diag is not None, first, last, ntp, heads,
                             dh ** -0.5, 128, 2048)
    extra = dict(collective_id=cid, has_side_effects=True) if ntp > 1 else {}
    return pl.pallas_call(
        kern, grid=(steps,), in_specs=specs, out_specs=out_specs, out_shape=out_shape, scratch_shapes=scratch,
        cost_estimate=pl.CostEstimate(flops=8 * n * hd * keys, bytes_accessed=4 * keys * 256, transcendentals=0),
        compiler_params=pltpu.CompilerParams(vmem_limit_bytes=60 * 1024 * 1024, **extra),
        name="attn_last" if last else "attn_first",
    )(*args)


def proj_kernel(a_ref, w_ref, x_ref, out_ref):
    y = jnp.dot(a_ref[...], w_ref[...], preferred_element_type=jnp.float32)
    out_ref[...] = x_ref[...] + y.astype(jnp.bfloat16)


def proj(a, w, x):
    n, k = a.shape
    d = w.shape[1]
    nc = 256
    col = pl.BlockSpec((n, nc), lambda i: (0, i))
    return pl.pallas_call(
        proj_kernel, grid=(d // nc,),
        in_specs=[pl.BlockSpec(memory_space=pltpu.VMEM), pl.BlockSpec((k, nc), lambda i: (0, i)), col],
        out_specs=col, out_shape=jax.ShapeDtypeStruct((n, d), jnp.bfloat16),
        cost_estimate=pl.CostEstimate(flops=2 * n * k * d, bytes_accessed=2 * k * d, transcendentals=0),
        compiler_params=pltpu.CompilerParams(vmem_limit_bytes=48 * 1024 * 1024),
        name="proj",
    )(a, w, x)


def sum_kernel(ntp, nb, rsplit, skew, a_ref, w_ref, x_ref, out_ref, p_ref, ra, rb_, ga, gb, send_sem, recv_sem):
    z = lax.axis_index("tp")
    s = pl.program_id(0)
    nc = w_ref.shape[1]
    half = a_ref.shape[0] // 2
    rows = half // rsplit
    nchunk = nb * rsplit
    last = ntp - 1

    @pl.when(s == 0)
    def _():
        bar = pltpu.get_barrier_semaphore()

        @pl.when(z > 0)
        def _():
            pl.semaphore_signal(bar, inc=1, device_id={"tp": z - 1}, device_id_type=MESH)

        @pl.when(z < last)
        def _():
            pl.semaphore_signal(bar, inc=1, device_id={"tp": z + 1}, device_id_type=MESH)

        @pl.when((z > 0) & (z < last))
        def _():
            pl.semaphore_wait(bar, 2)

        @pl.when((z == 0) | (z == last))
        def _():
            pl.semaphore_wait(bar, 1)

    @pl.when((s < nchunk) & (s % rsplit == 0))
    def _():
        p = jnp.dot(a_ref[...], w_ref[...], preferred_element_type=jnp.float32)
        for h in range(2):
            for r in range(rsplit):
                lo = h * half + r * rows
                p_ref[h, s + r] = p[lo:lo + rows, :]

    def copy(kind, src, dst, c, to):
        return pltpu.make_async_remote_copy(
            src_ref=src.at[c], dst_ref=dst.at[c], send_sem=send_sem.at[kind, c], recv_sem=recv_sem.at[kind, c],
            device_id={"tp": to}, device_id_type=MESH)

    def side(h, red, gat):
        d = (last - z) if h == 0 else z
        to_end = (z - 1) if h == 0 else (z + 1)
        from_end = (z + 1) if h == 0 else (z - 1)

        def store(c, v):
            col = pl.multiple_of((c // rsplit) * nc, nc)
            row = pl.multiple_of(h * half + (c % rsplit) * rows, rows)
            out_ref[pl.ds(row, rows), pl.ds(col, nc)] = v

        c = s - skew * d

        @pl.when((c >= 0) & (c < nchunk))
        def _():
            @pl.when(d == 0)
            def _():
                copy(h, p_ref.at[h], red, c, to_end).start()

            @pl.when((d > 0) & (d < last))
            def _():
                copy(h, red, red, c, to_end).wait_recv()
                red[c] = red[c] + p_ref[h, c]
                copy(h, red, red, c, to_end).start()

            @pl.when(d == last)
            def _():
                copy(h, red, red, c, from_end).wait_recv()
                col = pl.multiple_of((c // rsplit) * nc, nc)
                row = pl.multiple_of(h * half + (c % rsplit) * rows, rows)
                y = (red[c] + p_ref[h, c]).astype(jnp.bfloat16)
                xn = x_ref[pl.ds(row, rows), pl.ds(col, nc)] + y
                gat[c] = xn
                copy(2 + h, gat, gat, c, from_end).start()
                store(c, xn)

        e = s - skew * (2 * last - d)

        @pl.when((e >= 0) & (e < nchunk) & (d < last))
        def _():
            copy(2 + h, gat, gat, e, from_end).wait_recv()

            @pl.when(d > 0)
            def _():
                copy(2 + h, gat, gat, e, from_end).start()

            store(e, gat[e])

    side(0, ra, ga)
    side(1, rb_, gb)

    @pl.when(s == pl.num_programs(0) - 1)
    def _():
        def body(c, _):
            for h, (red, gat) in enumerate(((ra, ga), (rb_, gb))):
                d = (last - z) if h == 0 else z
                to_end = (z - 1) if h == 0 else (z + 1)
                from_end = (z + 1) if h == 0 else (z - 1)

                @pl.when(d < last)
                def _():
                    copy(h, red, red, c, to_end).wait_send()

                @pl.when(d > 0)
                def _():
                    copy(2 + h, gat, gat, c, from_end).wait_send()
            return 0

        lax.fori_loop(0, nchunk, body, 0)


def matmul_sum(a, w, layer, x, ntp, cid):
    n, k = a.shape
    d = w.shape[2]
    nc, rsplit, skew = 256, 2, 2
    nb = d // nc
    nchunk = nb * rsplit
    rows = n // 2 // rsplit
    steps = nchunk + 2 * (ntp - 1) * skew
    kern = functools.partial(sum_kernel, ntp, nb, rsplit, skew)
    vm = pl.BlockSpec(memory_space=pltpu.VMEM)
    f32, bf = jnp.float32, jnp.bfloat16
    return pl.pallas_call(
        kern, grid=(steps,),
        in_specs=[vm, pl.BlockSpec((None, k, nc), lambda s: (layer, 0, jnp.minimum(s // rsplit, nb - 1))), vm],
        out_specs=vm,
        out_shape=jax.ShapeDtypeStruct((n, d), bf),
        scratch_shapes=[
            pltpu.VMEM((2, nchunk, rows, nc), f32),
            pltpu.VMEM((nchunk, rows, nc), f32),
            pltpu.VMEM((nchunk, rows, nc), f32),
            pltpu.VMEM((nchunk, rows, nc), bf),
            pltpu.VMEM((nchunk, rows, nc), bf),
            pltpu.SemaphoreType.DMA((4, nchunk)),
            pltpu.SemaphoreType.DMA((4, nchunk)),
        ],
        cost_estimate=pl.CostEstimate(flops=100_000_000_000, bytes_accessed=2 * k * d, transcendentals=0),
        compiler_params=pltpu.CompilerParams(
            collective_id=cid, has_side_effects=True, vmem_limit_bytes=62 * 1024 * 1024),
        name="matmul_sum",
    )(a, w, x)


def solution(mesh):
    sp = mesh.shape['sp']
    tp = mesh.shape['tp']
    row = ('dp', 'sp')
    kv_spec = P(None, row, 'tp', None)
    col = P(None, None, 'tp')
    rowsplit = P(None, 'tp', None)

    def xchg(t, bit):
        return lax.ppermute(t, 'sp', [(i, i ^ bit) for i in range(sp)])

    def body(x, pos, k_hist, v_hist, wq, wk, wv, wo, wg, wu, wd, g1, g2):
        n, d = x.shape
        layers, t, kvl, dh = k_hist.shape
        hql = wq.shape[-1] // dh
        g = hql // kvl
        idx = lax.axis_index('sp')
        src = jnp.arange(3 * n, dtype=jnp.int32)[None, :] // n + 1
        bias = jnp.where((idx ^ src) < idx, 0.0, -jnp.inf).astype(jnp.float32)
        bias = jnp.broadcast_to(bias, (8, 3 * n))
        tabs = rope_tables(pos, dh)
        plane = lax.axis_index('dp') * sp + idx
        nplane = mesh.shape['dp'] * sp
        plane = lax.axis_index('dp') * sp + idx
        nplane = mesh.shape['dp'] * sp
        raw = [(k_hist[l].reshape(t, kvl * dh), v_hist[l].reshape(t, kvl * dh)) for l in range(layers)]

        def fetch(k0, v0):
            k1, v1 = xchg(k0, 1), xchg(v0, 1)
            k2, v2 = xchg(k0, 2), xchg(v0, 2)
            return k1, v1, k2, v2

        def whole_wo(l):
            part = lax.dynamic_slice(wo, (l, plane * dh, 0), (1, dh, d))[0]
            w = lax.all_gather(part, 'tp', axis=0)
            return lax.all_gather(w, ('dp', 'sp'), axis=0).reshape(tp * hql * dh, d)

        near = fetch(*raw[0])
        full_wo = {l: whole_wo(l) for l in range(1, layers)} if nplane == hql else {}
        far = None
        ks, vs = [], []
        for l in range(layers):
            k0, v0 = raw[l]
            k1, v1, k2, v2 = near
            q, k, v = qkv(x, g1[l:l + 1], *tabs, wq, wk, wv, l, dh)
            ks.append(k.reshape(n, kvl, dh))
            vs.append(v.reshape(n, kvl, dh))
            n1, w1 = xchg(k, 1), xchg(v, 1)
            n2, w2 = xchg(k, 2), xchg(v, 2)
            st = attention(bias, q, [(k0, v0), (k1, v1)], (k, v), [], None, False, g)
            k2, v2, n2, w2, st = lax.optimization_barrier((k2, v2, n2, w2, st))
            k3, v3 = far if far is not None else (xchg(k2, 1), xchg(v2, 1))
            n3, w3 = xchg(n2, 1), xchg(w2, 1)
            late = [(jnp.concatenate([n1, n2, n3]), jnp.concatenate([w1, w2, w3]))]
            last = [(k2, v2), (k3, v3)]
            more = l + 1 < layers
            net = (tp, 2 * l) if l in full_wo else ()
            attn = attention(bias, q, last, None, late, st, True, g, *net)
            if more:
                *raw[l + 1], attn = lax.optimization_barrier((*raw[l + 1], attn))
                near = fetch(*raw[l + 1])
            x = proj(attn, full_wo[l], x) if l in full_wo else matmul_sum(attn, wo, l, x, tp, 2 * l)
            if more:
                *near, x = lax.optimization_barrier((*near, x))
                far = xchg(near[2], 1), xchg(near[3], 1)
            u = gate_up(x, g2[l:l + 1], wg, wu, l)
            if more:
                *far, u = lax.optimization_barrier((*far, u))
            x = matmul_sum(u, wd, l, x, tp, 2 * l + 1)
        return x, jnp.stack(ks), jnp.stack(vs)

    in_specs = (P(row, None), P(row), kv_spec, kv_spec, col, col, col, rowsplit, col, col, rowsplit, P(), P())
    out_specs = (P(row, None), kv_spec, kv_spec)
    return jax.shard_map(body, mesh=mesh, in_specs=in_specs, out_specs=out_specs, check_vma=False)
```

```python
import functools

import jax
import jax.numpy as jnp
from jax import lax
from jax.experimental import pallas as pl
from jax.experimental.pallas import tpu as pltpu
from jax.sharding import PartitionSpec as P


EPS = 1e-5
ROPE_THETA = 500000.0
MESH = pl.DeviceIdType.MESH
LOG2E = 1.4426950408889634


def rope_tables(pos, dh):
    half = dh // 2
    inv = ROPE_THETA ** (-(jnp.arange(half, dtype=jnp.float32) * (2.0 / dh)))
    ang = pos.astype(jnp.float32)[:, None] * inv
    c, s = jnp.cos(ang), jnp.sin(ang)
    return jnp.concatenate([c, c], -1), jnp.concatenate([-s, s], -1)


def norm_into(x_ref, g_ref, h_ref):
    rb = 64
    for lo in range(0, x_ref.shape[0], rb):
        xf = x_ref[lo:lo + rb, :].astype(jnp.float32)
        r = lax.rsqrt(jnp.mean(xf * xf, axis=-1, keepdims=True) + EPS)
        h_ref[lo:lo + rb, :] = (xf * r * g_ref[...].astype(jnp.float32)).astype(jnp.bfloat16)


def qkv_kernel(nq, dh, x_ref, g_ref, c_ref, s_ref, wq_ref, wk_ref, wv_ref, q_ref, k_ref, v_ref, h_ref):
    i = pl.program_id(0)

    @pl.when(i == 0)
    def _():
        norm_into(x_ref, g_ref, h_ref)

    def rotated(w_ref, out):
        t = jnp.dot(h_ref[...], w_ref[...], preferred_element_type=jnp.float32)
        t = t.astype(jnp.bfloat16).astype(jnp.float32)
        for j in range(t.shape[1] // dh):
            th = t[:, j * dh:(j + 1) * dh]
            r = th * c_ref[...] + pltpu.roll(th, dh // 2, 1) * s_ref[...]
            out[:, j * dh:(j + 1) * dh] = r.astype(jnp.bfloat16)

    @pl.when(i < nq)
    def _():
        rotated(wq_ref, q_ref)

    @pl.when(i == nq)
    def _():
        rotated(wk_ref, k_ref)

    @pl.when(i == nq + 1)
    def _():
        v_ref[...] = jnp.dot(h_ref[...], wv_ref[...], preferred_element_type=jnp.float32).astype(jnp.bfloat16)


def qkv(x, g, c, s, wq, wk, wv, layer, dh):
    n, d = x.shape
    hq, hk = wq.shape[2], wk.shape[2]
    nc = 256
    nq = hq // nc
    vm = pl.BlockSpec(memory_space=pltpu.VMEM)
    bf = jnp.bfloat16
    return pl.pallas_call(
        functools.partial(qkv_kernel, nq, dh), grid=(nq + 2,),
        in_specs=[vm, vm, vm, vm,
                  pl.BlockSpec((None, d, nc), lambda i: (layer, 0, jnp.minimum(i, nq - 1))),
                  pl.BlockSpec((None, d, hk), lambda i: (layer, 0, 0)),
                  pl.BlockSpec((None, d, hk), lambda i: (layer, 0, 0))],
        out_specs=[pl.BlockSpec((n, nc), lambda i: (0, jnp.minimum(i, nq - 1))), vm, vm],
        out_shape=[jax.ShapeDtypeStruct((n, hq), bf), jax.ShapeDtypeStruct((n, hk), bf),
                   jax.ShapeDtypeStruct((n, hk), bf)],
        scratch_shapes=[pltpu.VMEM((n, d), bf)],
        cost_estimate=pl.CostEstimate(flops=2 * n * d * (hq + 2 * hk), bytes_accessed=2 * d * hq, transcendentals=0),
        compiler_params=pltpu.CompilerParams(vmem_limit_bytes=48 * 1024 * 1024),
        name="qkv",
    )(x, g, c, s, wq, wk, wv)


def gate_kernel(x_ref, g_ref, wg_ref, wu_ref, u_ref, h_ref):
    @pl.when(pl.program_id(0) == 0)
    def _():
        norm_into(x_ref, g_ref, h_ref)

    a = jnp.dot(h_ref[...], wg_ref[...], preferred_element_type=jnp.float32)
    b = jnp.dot(h_ref[...], wu_ref[...], preferred_element_type=jnp.float32)
    a = a.astype(jnp.bfloat16).astype(jnp.float32)
    b = b.astype(jnp.bfloat16).astype(jnp.float32)
    u_ref[...] = (jax.nn.silu(a) * b).astype(jnp.bfloat16)


def gate_up(x, g, wg, wu, layer):
    n, d = x.shape
    f = wg.shape[2]
    nc = 256
    vm = pl.BlockSpec(memory_space=pltpu.VMEM)
    wspec = pl.BlockSpec((None, d, nc), lambda i: (layer, 0, i))
    return pl.pallas_call(
        gate_kernel, grid=(f // nc,), in_specs=[vm, vm, wspec, wspec],
        out_specs=pl.BlockSpec((n, nc), lambda i: (0, i)),
        out_shape=jax.ShapeDtypeStruct((n, f), jnp.bfloat16),
        scratch_shapes=[pltpu.VMEM((n, d), jnp.bfloat16)],
        cost_estimate=pl.CostEstimate(flops=4 * n * d * f, bytes_accessed=4 * d * f, transcendentals=0),
        compiler_params=pltpu.CompilerParams(vmem_limit_bytes=48 * 1024 * 1024),
        name="gate_up",
    )(x, g, wg, wu)


def attn_kernel(nfull, ncond, diag, first, last, ntp, heads, scale, rb, tk, *refs):
    it = iter(refs)
    bias = next(it)
    q_ref = next(it)
    full = [(next(it), next(it)) for _ in range(nfull)]
    own = (next(it), next(it)) if diag else None
    cond = [(next(it), next(it)) for _ in range(ncond)]
    if not first:
        m_in, l_in, o_in = next(it), next(it), next(it)
    out = next(it)
    if not last:
        m_s, l_s, o_s = out, next(it), next(it)
    nq = q_ref.shape[0]
    rows = range(0, nq, rb)

    def logits(t):
        lo, k_ref, _, off, size, _ = t
        s = lax.dot_general(q_ref[lo:lo + rb, :], k_ref[off:off + size, :], (((1,), (1,)), ((), ())),
                            preferred_element_type=jnp.float32)
        return s * (scale * LOG2E)

    def absorb(t, s, st):
        lo, _, v_ref, off, size, mask = t
        if mask == "causal":
            r = lax.broadcasted_iota(jnp.int32, s.shape, 0) + lo
            c = lax.broadcasted_iota(jnp.int32, s.shape, 1) + off
            s = jnp.where(c <= r, s, -jnp.inf)
        elif mask == "bias":
            s = s + bias[:1, off:off + size]
        mx = jnp.max(s, axis=-1, keepdims=True)
        if st is not None:
            mx = jnp.maximum(mx, st[0])
        p = jnp.exp2(s - mx)
        ps = jnp.sum(p, axis=-1, keepdims=True)
        o = jnp.dot(p.astype(jnp.bfloat16), v_ref[off:off + size, :], preferred_element_type=jnp.float32)
        if st is not None:
            al = jnp.exp2(st[0] - mx)
            ps = ps + al * st[1]
            o = o + al * st[2]
        return mx, ps, o

    def one_head(put):
        st = {lo: None for lo in rows}
        if not first:
            st = {lo: (m_in[lo:lo + rb, :1], l_in[lo:lo + rb, :1], o_in[lo:lo + rb, :]) for lo in rows}
        tiles = [(lo, k, v, off, tk, None) for k, v in full for off in range(0, k.shape[0], tk) for lo in rows]
        if diag:
            tiles += [(lo, own[0], own[1], 0, lo + rb, "causal") for lo in rows]
        tiles += [(lo, k, v, 0, k.shape[0], "bias") for k, v in cond for lo in rows]
        s_next = logits(tiles[0])
        for i, t in enumerate(tiles):
            s = s_next
            if i + 1 < len(tiles):
                s_next = logits(tiles[i + 1])
            st[t[0]] = absorb(t, s, st[t[0]])
        for lo in rows:
            m, l, o = st[lo]
            if last:
                put(lo, (o / l).astype(jnp.bfloat16))
            else:
                m_s[lo:lo + rb, :] = jnp.broadcast_to(m, (rb, 128))
                l_s[lo:lo + rb, :] = jnp.broadcast_to(l, (rb, 128))
                o_s[lo:lo + rb, :] = o

    if ntp == 1:
        def put(lo, v):
            out[lo:lo + rb, :] = v

        one_head(put)
        return

    buf, send_r, send_l, recv_r, recv_l = [next(it) for _ in range(5)]
    z = lax.axis_index("tp")
    step = pl.program_id(0)
    end = ntp - 1
    dh = q_ref.shape[1]

    @pl.when(step == 0)
    def _():
        bar = pltpu.get_barrier_semaphore()

        @pl.when(z > 0)
        def _():
            pl.semaphore_signal(bar, inc=1, device_id={"tp": z - 1}, device_id_type=MESH)

        @pl.when(z < end)
        def _():
            pl.semaphore_signal(bar, inc=1, device_id={"tp": z + 1}, device_id_type=MESH)

        @pl.when((z > 0) & (z < end))
        def _():
            pl.semaphore_wait(bar, 2)

        @pl.when((z == 0) | (z == end))
        def _():
            pl.semaphore_wait(bar, 1)

    def rightwards(src, h):
        return pltpu.make_async_remote_copy(
            src_ref=buf.at[src, h], dst_ref=buf.at[src, h], send_sem=send_r.at[src, h], recv_sem=recv_r.at[src, h],
            device_id={"tp": z + 1}, device_id_type=MESH)

    def leftwards(src, h):
        return pltpu.make_async_remote_copy(
            src_ref=buf.at[src, h], dst_ref=buf.at[src, h], send_sem=send_l.at[src, h], recv_sem=recv_l.at[src, h],
            device_id={"tp": z - 1}, device_id_type=MESH)

    def emit(src, h):
        col = pl.multiple_of((h * ntp + src) * dh, dh)
        out[:, pl.ds(col, dh)] = buf[src, h]

    @pl.when(step < heads)
    def _():
        def put(lo, v):
            buf[z, step, lo:lo + rb, :] = v

        one_head(put)

        @pl.when(z < end)
        def _():
            rightwards(z, step).start()

        @pl.when(z > 0)
        def _():
            leftwards(z, step).start()

        emit(z, step)

    for k in range(1, ntp):
        c = step - k
        live = (c >= 0) & (c < heads)

        @pl.when(live & (z - k >= 0))
        def _():
            rightwards(z - k, c).wait_recv()

            @pl.when(z < end)
            def _():
                rightwards(z - k, c).start()

            emit(z - k, c)

        @pl.when(live & (z + k <= end))
        def _():
            leftwards(z + k, c).wait_recv()

            @pl.when(z > 0)
            def _():
                leftwards(z + k, c).start()

            emit(z + k, c)

    @pl.when(step == pl.num_programs(0) - 1)
    def _():
        def body(h, _):
            for src in range(ntp):
                @pl.when((z >= src) & (z < end))
                def _():
                    rightwards(src, h).wait_send()

                @pl.when((z <= src) & (z > 0))
                def _():
                    leftwards(src, h).wait_send()
            return 0

        lax.fori_loop(0, heads, body, 0)


def attention(bias, q, full, diag, cond, state, last, g, ntp=1, cid=None):
    n, hd = q.shape
    dh = 128
    heads = hd // dh
    first = state is None
    steps = heads if ntp == 1 else heads + ntp - 1
    at = lambda h: jnp.minimum(h, heads - 1)
    args = [bias, q]
    specs = [pl.BlockSpec(memory_space=pltpu.VMEM), pl.BlockSpec((n, dh), lambda h: (0, at(h)))]
    kvspec = lambda t: pl.BlockSpec((t, dh), lambda h: (0, at(h) // g))
    keys = 0
    for k, v in full + ([diag] if diag is not None else []) + cond:
        args += [k, v]
        specs += [kvspec(k.shape[0])] * 2
        keys += k.shape[0]
    hspec = pl.BlockSpec((n, dh), lambda h: (0, at(h)))
    f32 = jax.ShapeDtypeStruct((n, hd), jnp.float32)
    if not first:
        args += list(state)
        specs += [hspec] * 3
    scratch = []
    if ntp > 1:
        out_shape = jax.ShapeDtypeStruct((n, hd * ntp), jnp.bfloat16)
        out_specs = pl.BlockSpec(memory_space=pltpu.VMEM)
        scratch = [pltpu.VMEM((ntp, heads, n, dh), jnp.bfloat16)] + [pltpu.SemaphoreType.DMA((ntp, heads))] * 4
    elif last:
        out_shape, out_specs = jax.ShapeDtypeStruct((n, hd), jnp.bfloat16), hspec
    else:
        out_shape, out_specs = (f32,) * 3, (hspec,) * 3
    kern = functools.partial(attn_kernel, len(full), len(cond), diag is not None, first, last, ntp, heads,
                             dh ** -0.5, 128, 2048)
    extra = dict(collective_id=cid, has_side_effects=True) if ntp > 1 else {}
    return pl.pallas_call(
        kern, grid=(steps,), in_specs=specs, out_specs=out_specs, out_shape=out_shape, scratch_shapes=scratch,
        cost_estimate=pl.CostEstimate(flops=8 * n * hd * keys, bytes_accessed=4 * keys * 256, transcendentals=0),
        compiler_params=pltpu.CompilerParams(vmem_limit_bytes=60 * 1024 * 1024, **extra),
        name="attn_last" if last else "attn_first",
    )(*args)


def proj_kernel(a_ref, w_ref, x_ref, out_ref):
    y = jnp.dot(a_ref[...], w_ref[...], preferred_element_type=jnp.float32)
    out_ref[...] = x_ref[...] + y.astype(jnp.bfloat16)


def proj(a, w, x):
    n, k = a.shape
    d = w.shape[1]
    nc = 512
    col = pl.BlockSpec((n, nc), lambda i: (0, i))
    return pl.pallas_call(
        proj_kernel, grid=(d // nc,),
        in_specs=[pl.BlockSpec(memory_space=pltpu.VMEM), pl.BlockSpec((k, nc), lambda i: (0, i)), col],
        out_specs=col, out_shape=jax.ShapeDtypeStruct((n, d), jnp.bfloat16),
        cost_estimate=pl.CostEstimate(flops=2 * n * k * d, bytes_accessed=2 * k * d, transcendentals=0),
        compiler_params=pltpu.CompilerParams(vmem_limit_bytes=48 * 1024 * 1024),
        name="proj",
    )(a, w, x)


def sum_kernel(ntp, nb, rsplit, skew, a_ref, w_ref, x_ref, out_ref, p_ref, ra, rb_, ga, gb, send_sem, recv_sem):
    z = lax.axis_index("tp")
    s = pl.program_id(0)
    nc = w_ref.shape[1]
    half = a_ref.shape[0] // 2
    rows = half // rsplit
    nchunk = nb * rsplit
    last = ntp - 1

    @pl.when(s == 0)
    def _():
        bar = pltpu.get_barrier_semaphore()

        @pl.when(z > 0)
        def _():
            pl.semaphore_signal(bar, inc=1, device_id={"tp": z - 1}, device_id_type=MESH)

        @pl.when(z < last)
        def _():
            pl.semaphore_signal(bar, inc=1, device_id={"tp": z + 1}, device_id_type=MESH)

        @pl.when((z > 0) & (z < last))
        def _():
            pl.semaphore_wait(bar, 2)

        @pl.when((z == 0) | (z == last))
        def _():
            pl.semaphore_wait(bar, 1)

    @pl.when((s < nchunk) & (s % rsplit == 0))
    def _():
        p = jnp.dot(a_ref[...], w_ref[...], preferred_element_type=jnp.float32)
        for h in range(2):
            for r in range(rsplit):
                lo = h * half + r * rows
                p_ref[h, s + r] = p[lo:lo + rows, :]

    def copy(kind, src, dst, c, to):
        return pltpu.make_async_remote_copy(
            src_ref=src.at[c], dst_ref=dst.at[c], send_sem=send_sem.at[kind, c], recv_sem=recv_sem.at[kind, c],
            device_id={"tp": to}, device_id_type=MESH)

    def side(h, red, gat):
        d = (last - z) if h == 0 else z
        to_end = (z - 1) if h == 0 else (z + 1)
        from_end = (z + 1) if h == 0 else (z - 1)

        def store(c, v):
            col = pl.multiple_of((c // rsplit) * nc, nc)
            row = pl.multiple_of(h * half + (c % rsplit) * rows, rows)
            out_ref[pl.ds(row, rows), pl.ds(col, nc)] = v

        c = s - skew * d

        @pl.when((c >= 0) & (c < nchunk))
        def _():
            @pl.when(d == 0)
            def _():
                copy(h, p_ref.at[h], red, c, to_end).start()

            @pl.when((d > 0) & (d < last))
            def _():
                copy(h, red, red, c, to_end).wait_recv()
                red[c] = red[c] + p_ref[h, c]
                copy(h, red, red, c, to_end).start()

            @pl.when(d == last)
            def _():
                copy(h, red, red, c, from_end).wait_recv()
                col = pl.multiple_of((c // rsplit) * nc, nc)
                row = pl.multiple_of(h * half + (c % rsplit) * rows, rows)
                y = (red[c] + p_ref[h, c]).astype(jnp.bfloat16)
                xn = x_ref[pl.ds(row, rows), pl.ds(col, nc)] + y
                gat[c] = xn
                copy(2 + h, gat, gat, c, from_end).start()
                store(c, xn)

        e = s - skew * (2 * last - d)

        @pl.when((e >= 0) & (e < nchunk) & (d < last))
        def _():
            copy(2 + h, gat, gat, e, from_end).wait_recv()

            @pl.when(d > 0)
            def _():
                copy(2 + h, gat, gat, e, from_end).start()

            store(e, gat[e])

    side(0, ra, ga)
    side(1, rb_, gb)

    @pl.when(s == pl.num_programs(0) - 1)
    def _():
        def body(c, _):
            for h, (red, gat) in enumerate(((ra, ga), (rb_, gb))):
                d = (last - z) if h == 0 else z
                to_end = (z - 1) if h == 0 else (z + 1)
                from_end = (z + 1) if h == 0 else (z - 1)

                @pl.when(d < last)
                def _():
                    copy(h, red, red, c, to_end).wait_send()

                @pl.when(d > 0)
                def _():
                    copy(2 + h, gat, gat, c, from_end).wait_send()
            return 0

        lax.fori_loop(0, nchunk, body, 0)


def matmul_sum(a, w, layer, x, ntp, cid):
    n, k = a.shape
    d = w.shape[2]
    nc, rsplit, skew = 256, 2, 2
    nb = d // nc
    nchunk = nb * rsplit
    rows = n // 2 // rsplit
    steps = nchunk + 2 * (ntp - 1) * skew
    kern = functools.partial(sum_kernel, ntp, nb, rsplit, skew)
    vm = pl.BlockSpec(memory_space=pltpu.VMEM)
    f32, bf = jnp.float32, jnp.bfloat16
    return pl.pallas_call(
        kern, grid=(steps,),
        in_specs=[vm, pl.BlockSpec((None, k, nc), lambda s: (layer, 0, jnp.minimum(s // rsplit, nb - 1))), vm],
        out_specs=vm,
        out_shape=jax.ShapeDtypeStruct((n, d), bf),
        scratch_shapes=[
            pltpu.VMEM((2, nchunk, rows, nc), f32),
            pltpu.VMEM((nchunk, rows, nc), f32),
            pltpu.VMEM((nchunk, rows, nc), f32),
            pltpu.VMEM((nchunk, rows, nc), bf),
            pltpu.VMEM((nchunk, rows, nc), bf),
            pltpu.SemaphoreType.DMA((4, nchunk)),
            pltpu.SemaphoreType.DMA((4, nchunk)),
        ],
        cost_estimate=pl.CostEstimate(flops=100_000_000_000, bytes_accessed=2 * k * d, transcendentals=0),
        compiler_params=pltpu.CompilerParams(
            collective_id=cid, has_side_effects=True, vmem_limit_bytes=62 * 1024 * 1024),
        name="matmul_sum",
    )(a, w, x)


def solution(mesh):
    sp = mesh.shape['sp']
    tp = mesh.shape['tp']
    row = ('dp', 'sp')
    kv_spec = P(None, row, 'tp', None)
    col = P(None, None, 'tp')
    rowsplit = P(None, 'tp', None)

    def xchg(t, bit):
        return lax.ppermute(t, 'sp', [(i, i ^ bit) for i in range(sp)])

    def body(x, pos, k_hist, v_hist, wq, wk, wv, wo, wg, wu, wd, g1, g2):
        n, d = x.shape
        layers, t, kvl, dh = k_hist.shape
        hql = wq.shape[-1] // dh
        g = hql // kvl
        idx = lax.axis_index('sp')
        src = jnp.arange(3 * n, dtype=jnp.int32)[None, :] // n + 1
        bias = jnp.where((idx ^ src) < idx, 0.0, -jnp.inf).astype(jnp.float32)
        bias = jnp.broadcast_to(bias, (8, 3 * n))
        tabs = rope_tables(pos, dh)
        plane = lax.axis_index('dp') * sp + idx
        nplane = mesh.shape['dp'] * sp
        plane = lax.axis_index('dp') * sp + idx
        nplane = mesh.shape['dp'] * sp
        raw = [(k_hist[l].reshape(t, kvl * dh), v_hist[l].reshape(t, kvl * dh)) for l in range(layers)]

        def fetch(k0, v0):
            k1, v1 = xchg(k0, 1), xchg(v0, 1)
            k2, v2 = xchg(k0, 2), xchg(v0, 2)
            return k1, v1, k2, v2

        def whole_wo(l):
            part = lax.dynamic_slice(wo, (l, plane * dh, 0), (1, dh, d))[0]
            w = lax.all_gather(part, 'tp', axis=0)
            return lax.all_gather(w, ('dp', 'sp'), axis=0).reshape(tp * hql * dh, d)

        near = fetch(*raw[0])
        full_wo = {l: whole_wo(l) for l in range(1, layers)} if nplane == hql else {}
        far = None
        ks, vs = [], []
        for l in range(layers):
            k0, v0 = raw[l]
            k1, v1, k2, v2 = near
            q, k, v = qkv(x, g1[l:l + 1], *tabs, wq, wk, wv, l, dh)
            ks.append(k.reshape(n, kvl, dh))
            vs.append(v.reshape(n, kvl, dh))
            n1, w1 = xchg(k, 1), xchg(v, 1)
            n2, w2 = xchg(k, 2), xchg(v, 2)
            early = [(k0, v0)] if l in full_wo else [(k0, v0), (k1, v1)]
            st = attention(bias, q, early, (k, v), [], None, False, g)
            k2, v2, n2, w2, st = lax.optimization_barrier((k2, v2, n2, w2, st))
            k3, v3 = far if far is not None else (xchg(k2, 1), xchg(v2, 1))
            n3, w3 = xchg(n2, 1), xchg(w2, 1)
            late = [(jnp.concatenate([n1, n2, n3]), jnp.concatenate([w1, w2, w3]))]
            last = ([(k1, v1)] if l in full_wo else []) + [(k2, v2), (k3, v3)]
            more = l + 1 < layers
            net = (tp, 2 * l) if l in full_wo else ()
            attn = attention(bias, q, last, None, late, st, True, g, *net)
            if more:
                *raw[l + 1], attn = lax.optimization_barrier((*raw[l + 1], attn))
                near = fetch(*raw[l + 1])
            x = proj(attn, full_wo[l], x) if l in full_wo else matmul_sum(attn, wo, l, x, tp, 2 * l)
            if more:
                *near, x = lax.optimization_barrier((*near, x))
                far = xchg(near[2], 1), xchg(near[3], 1)
            u = gate_up(x, g2[l:l + 1], wg, wu, l)
            if more:
                *far, u = lax.optimization_barrier((*far, u))
            x = matmul_sum(u, wd, l, x, tp, 2 * l + 1)
        return x, jnp.stack(ks), jnp.stack(vs)

    in_specs = (P(row, None), P(row), kv_spec, kv_spec, col, col, col, rowsplit, col, col, rowsplit, P(), P())
    out_specs = (P(row, None), kv_spec, kv_spec)
    return jax.shard_map(body, mesh=mesh, in_specs=in_specs, out_specs=out_specs, check_vma=False)
```
